32 devices in a mesh: gr: 8 (over z, x), gc: 4 (over y, core).
Axes of the slice: x: 2, y: 2, z: 4, core: 2. Of those that a mesh axis runs over, the one named last changes fastest.
Arguments:
- orbitals: bfloat16 [1536, 16384], P(None, ('gr', 'gc')), may hold values from -0.046875 to 0.046875
- velocities: bfloat16 [1536, 16384], P(None, ('gr', 'gc')), may hold values from -40 to 40
Outputs:
- new_velocities: float32 [1536, 16384], P(None, ('gr', 'gc'))
- violations: float32 [1], replicated
The draws below stay inside these ranges and needn't reach their ends.
All inputs are finite; a program needn't handle non-finite values.
Results may differ from the reference program's by a relative error of at most 0.0018.
Values may be sent and summed in bfloat16 or wider, within the bound.
A program may use at most 64 MiB of HBM per device.

```python
import jax
import jax.numpy as jnp

M = 1536
ITERS = 1
GV = 16384


def draw_velocities(key, part):
    index = jnp.arange(M, dtype=jnp.float32)
    scale = jnp.exp(jnp.log(10.0) * index / (M - 1))
    base = jnp.clip(jax.random.normal(key, (M, GV), jnp.float32), -4.0, 4.0)
    return (base * scale[:, None]).astype(jnp.bfloat16)


def shard_levels(rng, extent, pieces, smallest, largest):
    loudness = 1.0
    for axis_at, shards_of in pieces:
        steps = jax.random.uniform(jax.random.fold_in(jax.random.fold_in(rng, 6), axis_at), (shards_of,), jnp.float32, smallest / len(pieces), largest / len(pieces))
        loudness = loudness * jnp.repeat(jnp.exp(steps), extent[axis_at] // shards_of).reshape((-1,) + (1,) * (len(extent) - 1 - axis_at))
    return loudness


def centred(rng, extent, scale, most, split=(), kind=jnp.bfloat16):
    entries = scale * jax.random.normal(rng, extent, jnp.float32)
    if split:
        entries = entries * shard_levels(rng, extent, split, -0.22, 0.18)
    return jnp.clip(entries, -most, most).astype(kind)


def setup_inputs(seed: int = 0) -> dict:
    splits = jax.random.split(jax.random.key(seed), 3)
    return {
        "orbitals": centred(splits[0], (M, GV), GV ** -0.5, 0.046875, ((1, 32),)),
        "velocities": draw_velocities(jax.random.fold_in(splits[2], 71), 0),
    }


def reference(orbitals, velocities):
    vel = velocities.astype(jnp.float32)
    measured = []
    for step in range(ITERS):
        vel_b = vel.astype(jnp.bfloat16)
        intersection = jnp.dot(orbitals, vel_b.T, preferred_element_type=jnp.float32)
        sym = intersection + intersection.T
        measured.append(jnp.sqrt(jnp.sum(sym * sym)) / M)
        sym_b = sym.astype(jnp.bfloat16)
        vel = vel - 0.5 * jnp.dot(sym_b, orbitals, preferred_element_type=jnp.float32)
    return (vel, jnp.stack(measured))
```

```python
import functools

import jax
import jax.numpy as jnp
from jax import lax
from jax.experimental import pallas as pl
from jax.experimental.pallas import tpu as pltpu
from jax.sharding import PartitionSpec as P

MESH = pl.DeviceIdType.MESH
T = 128
ROWS = 16
LANES = 3


def packed_blocks(count):
    blocks = [(i, i) for i in range(count)]
    return blocks + [(i, j) for i in range(count) for j in range(i + 1, count)]


def bits_of(size):
    return size.bit_length() - 1


def stages(gr, gc, n_gr, n_gc):
    def axis_bits(at, size, low):
        found = []
        here = (at // 2**low) % 2
        low_partner = at + (1 - 2 * here) * 2**low
        if low == 0:
            found.append((low_partner, here))
        top = bits_of(size) - 1
        values = [(at // 2**k) % 2 for k in range(top + 1)]
        for k in range(1, top + 1):
            above = values[k + 1] if k < top else 0
            gray = values[k] + above - 2 * values[k] * above
            partner = at
            for m in range(1, k + 1):
                partner = partner + (1 - 2 * values[m]) * 2**m
            found.append((partner, gray))
        return found

    in_gc = [((gr, p), v) for p, v in axis_bits(gc, n_gc, 0)]
    in_gr = [((p, gc), v) for p, v in axis_bits(gr, n_gr, 0)]
    return in_gc[:1], in_gc[1:] + in_gr


def kernel(n_gr, n_gc, lanes, orb, vel, sym, square, left, right, acc, out_buf, in_buf, whole, send_sem, recv_sem):
    gr, gc = lax.axis_index("gr"), lax.axis_index("gc")
    first, rest = stages(gr, gc, n_gr, n_gc)
    every = first + rest
    depth = len(every)
    count = orb.shape[0] // T
    blocks = packed_blocks(count)
    slot = {pair: at for at, pair in enumerate(blocks)}

    barrier = pltpu.get_barrier_semaphore()
    for partner, _ in every:
        pl.semaphore_signal(barrier, inc=1, device_id=partner, device_id_type=MESH)

    half = orb.shape[1]
    left[:, :half] = orb[...]
    left[:, half:] = vel[...]
    right[:, :half] = vel[...]
    right[:, half:] = orb[...]
    used = len(blocks) * T
    if acc.shape[0] > used:
        acc[used:, :] = jnp.zeros((acc.shape[0] - used, T), jnp.float32)

    for i in range(count):
        strip = lax.dot_general(
            left[i * T : (i + 1) * T, :],
            right[i * T :, :],
            (((1,), (1,)), ((), ())),
            preferred_element_type=jnp.float32,
        )
        for j in range(i, count):
            at = slot[(i, j)] * T
            acc[at : at + T, :] = strip[:, (j - i) * T : (j - i + 1) * T]

    pl.semaphore_wait(barrier, depth)

    def rows(start, size):
        return pl.ds(pl.multiple_of(start, ROWS), size)

    orders = []
    for lane in range(len(lanes)):
        turn = lane * len(rest) // len(lanes)
        orders.append(first + rest[turn:] + rest[:turn])
    at = [base for base, _ in lanes]
    sends = []

    def reduce_start(lane, step):
        base, size = lanes[lane]
        partner, value = orders[lane][step]
        size = size >> (step + 1)
        away = at[lane] + (1 - value) * size
        at[lane] = at[lane] + value * size
        landing = base + (lanes[lane][1] - 2 * size)
        out_buf[rows(away, size), :] = acc[rows(away, size), :].astype(jnp.bfloat16)
        copy = pltpu.make_async_remote_copy(
            src_ref=out_buf.at[rows(away, size), :],
            dst_ref=in_buf.at[pl.ds(landing, size), :],
            send_sem=send_sem.at[lane, step],
            recv_sem=recv_sem.at[lane, step],
            device_id=partner,
            device_id_type=MESH,
        )
        copy.start()
        sends.append(copy)
        return copy, landing, size

    flying = [reduce_start(lane, 0) for lane in range(len(lanes))]
    for step in range(depth):
        for lane in range(len(lanes)):
            copy, landing, size = flying[lane]
            copy.wait_recv()
            here = rows(at[lane], size)
            total = acc[here, :] + in_buf[landing : landing + size, :].astype(jnp.float32)
            if step + 1 < depth:
                acc[here, :] = total
                flying[lane] = reduce_start(lane, step + 1)
            else:
                whole[here, :] = total.astype(jnp.bfloat16)

    def gather_start(lane, step):
        base, size = lanes[lane]
        partner, value = orders[lane][step]
        size = size >> (step + 1)
        mine = rows(at[lane], size)
        at[lane] = at[lane] - value * size
        copy = pltpu.make_async_remote_copy(
            src_ref=whole.at[mine, :],
            dst_ref=whole.at[mine, :],
            send_sem=send_sem.at[lane, depth + step],
            recv_sem=recv_sem.at[lane, depth + step],
            device_id=partner,
            device_id_type=MESH,
        )
        copy.start()
        sends.append(copy)
        return copy

    flying = [gather_start(lane, depth - 1) for lane in range(len(lanes))]
    for step in range(depth - 2, -2, -1):
        for lane in range(len(lanes)):
            flying[lane].wait_recv()
            if step >= 0:
                flying[lane] = gather_start(lane, step)

    total = jnp.zeros((8, T), jnp.float32)
    for at_slot, (i, j) in enumerate(blocks):
        block = whole[at_slot * T : (at_slot + 1) * T, :]
        value = block.astype(jnp.float32)
        weight = 1.0 if i == j else 2.0
        total = total + weight * jnp.sum((value * value).reshape(T // 8, 8, T), axis=0)
        sym[i * T : (i + 1) * T, j * T : (j + 1) * T] = block
        if i != j:
            sym[j * T : (j + 1) * T, i * T : (i + 1) * T] = block.T
    square[...] = total
    for copy in sends:
        copy.wait_send()


def solution(mesh):
    n_gr, n_gc = mesh.shape["gr"], mesh.shape["gc"]
    devices = n_gr * n_gc

    def local(orbitals, velocities):
        total_rows, cols = orbitals.shape
        count = total_rows // T
        unit = ROWS * devices
        units = -(-(count * (count + 1) // 2 * T) // unit)
        lanes, base = [], 0
        for lane in range(LANES):
            size = (units * (lane + 1) // LANES - units * lane // LANES) * unit
            lanes.append((base, size))
            base += size
        depth = bits_of(devices)
        vmem = pl.BlockSpec(memory_space=pltpu.VMEM)
        sym, square = pl.pallas_call(
            functools.partial(kernel, n_gr, n_gc, lanes),
            out_shape=(
                jax.ShapeDtypeStruct((total_rows, total_rows), jnp.bfloat16),
                jax.ShapeDtypeStruct((8, T), jnp.float32),
            ),
            in_specs=[vmem, vmem],
            out_specs=(vmem, vmem),
            scratch_shapes=[
                pltpu.VMEM((total_rows, 2 * cols), jnp.bfloat16),
                pltpu.VMEM((total_rows, 2 * cols), jnp.bfloat16),
                pltpu.VMEM((base, T), jnp.float32),
                pltpu.VMEM((base, T), jnp.bfloat16),
                pltpu.VMEM((base, T), jnp.bfloat16),
                pltpu.VMEM((base, T), jnp.bfloat16),
                pltpu.SemaphoreType.DMA((LANES, 2 * depth)),
                pltpu.SemaphoreType.DMA((LANES, 2 * depth)),
            ],
            compiler_params=pltpu.CompilerParams(
                collective_id=0, has_side_effects=True, vmem_limit_bytes=60 * 2**20
            ),
        )(orbitals, velocities)
        violation = jnp.sqrt(jnp.sum(square)) / total_rows
        moved = jnp.dot(sym, orbitals, preferred_element_type=jnp.float32)
        return velocities.astype(jnp.float32) - 0.5 * moved, violation[None]

    spec = P(None, ("gr", "gc"))
    return jax.shard_map(
        local, mesh=mesh, in_specs=(spec, spec), out_specs=(spec, P()), check_vma=False
    )
```

```python
import functools

import jax
import jax.numpy as jnp
from jax import lax
from jax.experimental import pallas as pl
from jax.experimental.pallas import tpu as pltpu
from jax.sharding import PartitionSpec as P

MESH = pl.DeviceIdType.MESH
T = 128
ROWS = 16
BATCHES = 2
WEIGHTS = (3, 3, 4, 0)


def packed_blocks(count):
    return [(i, j) for i in range(count) for j in range(i, count)]


def bits_of(size):
    return size.bit_length() - 1


def stages(gr, gc, n_gr, n_gc):
    def axis_bits(at, size, low):
        found = []
        here = (at // 2**low) % 2
        low_partner = at + (1 - 2 * here) * 2**low
        if low == 0:
            found.append((low_partner, here))
        top = bits_of(size) - 1
        values = [(at // 2**k) % 2 for k in range(top + 1)]
        for k in range(1, top + 1):
            above = values[k + 1] if k < top else 0
            gray = values[k] + above - 2 * values[k] * above
            partner = at
            for m in range(1, k + 1):
                partner = partner + (1 - 2 * values[m]) * 2**m
            found.append((partner, gray))
        return found

    in_gc = [((gr, p), v) for p, v in axis_bits(gc, n_gc, 0)]
    in_gr = [((p, gc), v) for p, v in axis_bits(gr, n_gr, 0)]
    return in_gc[:1], in_gc[1:] + in_gr


def lane_orders(first, rest):
    early, last = rest[:-1], rest[-1:]
    orders = []
    for lane in range(len(WEIGHTS) - 1):
        turn = lane % len(early)
        orders.append(first + early[turn:] + early[:turn] + last)
    return orders + [first + last + early]


def kernel(
    n_gr, n_gc, lanes, orb, vel, new, norm,
    left, right, acc, out_buf, in_buf, whole, sym, send_sem, recv_sem,
):
    gr, gc = lax.axis_index("gr"), lax.axis_index("gc")
    first, rest = stages(gr, gc, n_gr, n_gc)
    every = first + rest
    depth = len(every)
    count = orb.shape[0] // T
    blocks = packed_blocks(count)
    slot = {pair: at for at, pair in enumerate(blocks)}
    used = len(blocks) * T

    barrier = pltpu.get_barrier_semaphore()
    for partner, _ in every:
        pl.semaphore_signal(barrier, inc=1, device_id=partner, device_id_type=MESH)

    half = orb.shape[1]
    left[:, :half] = orb[...]
    left[:, half:] = vel[...]
    right[:, :half] = vel[...]
    right[:, half:] = orb[...]
    if acc.shape[0] > used:
        acc[used:, :] = jnp.zeros((acc.shape[0] - used, T), jnp.float32)

    def rows(start, size):
        return pl.ds(pl.multiple_of(start, ROWS), size)

    by_kind = lane_orders(first, rest)
    orders = [by_kind[kind] for _, _, kind in lanes]
    at = [base for base, _, _ in lanes]
    sends = []
    flying = [None] * len(lanes)

    def reduce_start(lane, step):
        base, length, _ = lanes[lane]
        partner, value = orders[lane][step]
        size = length >> (step + 1)
        away = rows(at[lane] + (1 - value) * size, size)
        at[lane] = at[lane] + value * size
        landing = base + (length - 2 * size)
        out_buf[away, :] = acc[away, :].astype(jnp.bfloat16)
        copy = pltpu.make_async_remote_copy(
            src_ref=out_buf.at[away, :],
            dst_ref=in_buf.at[pl.ds(landing, size), :],
            send_sem=send_sem.at[lane, step],
            recv_sem=recv_sem.at[lane, step],
            device_id=partner,
            device_id_type=MESH,
        )
        copy.start()
        sends.append(copy)
        flying[lane] = (copy, landing, size)

    started = 0
    for i in range(count):
        strip = lax.dot_general(
            left[i * T : (i + 1) * T, :],
            right[i * T :, :],
            (((1,), (1,)), ((), ())),
            preferred_element_type=jnp.float32,
        )
        for j in range(i, count):
            here = slot[(i, j)] * T
            acc[here : here + T, :] = strip[:, (j - i) * T : (j - i + 1) * T]
        done = (slot[(i, count - 1)] + 1) * T if i + 1 < count else acc.shape[0]
        while started < len(lanes) and lanes[started][0] + lanes[started][1] <= done:
            if started == 0:
                pl.semaphore_wait(barrier, depth)
            reduce_start(started, 0)
            started += 1

    for step in range(depth):
        for lane in range(len(lanes)):
            copy, landing, size = flying[lane]
            copy.wait_recv()
            here = rows(at[lane], size)
            total = acc[here, :] + in_buf[landing : landing + size, :].astype(jnp.float32)
            if step + 1 < depth:
                acc[here, :] = total
                reduce_start(lane, step + 1)
            else:
                whole[here, :] = total.astype(jnp.bfloat16)

    def gather_start(lane, step):
        _, length, _ = lanes[lane]
        partner, value = orders[lane][step]
        size = length >> (step + 1)
        mine = rows(at[lane], size)
        at[lane] = at[lane] - value * size
        copy = pltpu.make_async_remote_copy(
            src_ref=whole.at[mine, :],
            dst_ref=whole.at[mine, :],
            send_sem=send_sem.at[lane, depth + step],
            recv_sem=recv_sem.at[lane, depth + step],
            device_id=partner,
            device_id_type=MESH,
        )
        copy.start()
        sends.append(copy)
        flying[lane] = copy

    for lane in range(len(lanes)):
        gather_start(lane, depth - 1)
    for step in range(depth - 2, -1, -1):
        for lane in range(len(lanes)):
            flying[lane].wait_recv()
            gather_start(lane, step)

    square = jnp.zeros((8, T), jnp.float32)
    unpacked = 0
    for lane, (base, length, _) in enumerate(lanes):
        flying[lane].wait_recv()
        while unpacked < len(blocks) and (unpacked + 1) * T <= base + length:
            i, j = blocks[unpacked]
            block = whole[unpacked * T : (unpacked + 1) * T, :]
            value = block.astype(jnp.float32)
            part = jnp.sum((value * value).reshape(T // 8, 8, T), axis=0)
            square = square + (part if i == j else 2.0 * part)
            sym[i * T : (i + 1) * T, j * T : (j + 1) * T] = block
            if i != j:
                sym[j * T : (j + 1) * T, i * T : (i + 1) * T] = block.T
            unpacked += 1
            if j + 1 == count and i % 2 == 1 or unpacked == len(blocks):
                strip = slice(i // 2 * 2 * T, (i + 1) * T)
                moved = jnp.dot(sym[strip, :], orb[...], preferred_element_type=jnp.float32)
                new[strip, :] = vel[strip, :].astype(jnp.float32) - 0.5 * moved
    norm[0] = jnp.sqrt(jnp.sum(square)) / orb.shape[0]
    for copy in sends:
        copy.wait_send()


def solution(mesh):
    n_gr, n_gc = mesh.shape["gr"], mesh.shape["gc"]
    devices = n_gr * n_gc

    def local(orbitals, velocities):
        total_rows, cols = orbitals.shape
        count = total_rows // T
        unit = ROWS * devices
        units = -(-(count * (count + 1) // 2 * T) // unit)
        weights = WEIGHTS * BATCHES
        lanes, base, given = [], 0, 0
        for lane, weight in enumerate(weights):
            given += weight
            size = units * given // sum(weights) * unit - base
            if size:
                lanes.append((base, size, lane % len(WEIGHTS)))
            base += size
        depth = bits_of(devices)
        vmem = pl.BlockSpec(memory_space=pltpu.VMEM)
        return pl.pallas_call(
            functools.partial(kernel, n_gr, n_gc, lanes),
            out_shape=(
                jax.ShapeDtypeStruct((total_rows, cols), jnp.float32),
                jax.ShapeDtypeStruct((1,), jnp.float32),
            ),
            in_specs=[vmem, vmem],
            out_specs=(vmem, pl.BlockSpec(memory_space=pltpu.SMEM)),
            scratch_shapes=[
                pltpu.VMEM((total_rows, 2 * cols), jnp.bfloat16),
                pltpu.VMEM((total_rows, 2 * cols), jnp.bfloat16),
                pltpu.VMEM((base, T), jnp.float32),
                pltpu.VMEM((base, T), jnp.bfloat16),
                pltpu.VMEM((base, T), jnp.bfloat16),
                pltpu.VMEM((base, T), jnp.bfloat16),
                pltpu.VMEM((total_rows, total_rows), jnp.bfloat16),
                pltpu.SemaphoreType.DMA((len(lanes), 2 * depth)),
                pltpu.SemaphoreType.DMA((len(lanes), 2 * depth)),
            ],
            compiler_params=pltpu.CompilerParams(
                collective_id=0, has_side_effects=True, vmem_limit_bytes=34 * 2**20
            ),
        )(orbitals, velocities)

    spec = P(None, ("gr", "gc"))
    return jax.shard_map(
        local, mesh=mesh, in_specs=(spec, spec), out_specs=(spec, P()), check_vma=False
    )
```
